32 devices in a mesh: section: 4 (over y, x), fsdp: 8 (over z, core).
Axes of the slice: x: 2, y: 2, z: 4, core: 2. Of those that a mesh axis runs over, the one named last changes fastest.
Arguments:
- grad_parts: bfloat16 [4, 8, 8192, 1024], P('section', 'fsdp'), may hold values from -510 to 510
- first_codes: int32 [4, 8192, 1024], P('section', 'fsdp'), may hold values from -7 to 7
- first_rows: float32 [4, 8192], P('section', 'fsdp'), may hold values from 0.003 to 0.03
- first_columns: float32 [4, 1024], P('section'), may hold values from 0.003 to 0.03
- second_codes: int32 [4, 8192, 1024], P('section', 'fsdp'), may hold values from 1 to 15
- second_rows: float32 [4, 8192], P('section', 'fsdp'), may hold values from 0.001 to 0.01
- second_columns: float32 [4, 1024], P('section'), may hold values from 0.001 to 0.01
Outputs:
- direction: float32 [4, 8192, 1024], P('section', 'fsdp')
- first_scaled: float32 [4, 8192, 1024], P('section', 'fsdp')
- second_scaled: float32 [4, 8192, 1024], P('section', 'fsdp')
- first_rowmax: float32 [4, 8192], P('section', 'fsdp')
- first_colmax: float32 [4, 1024], P('section')
- second_rowmax: float32 [4, 8192], P('section', 'fsdp')
- second_colmax: float32 [4, 1024], P('section')
The draws below stay inside these ranges and needn't reach their ends.
All inputs are finite; a program needn't handle non-finite values. Where the reference program divides by a largest or mean magnitude, that divisor is 1e-20 or more.
Results may differ from the reference program's by a relative error of at most 0.0003.
Values may be sent and summed in bfloat16 or wider, within the bound.
A program may use at most 192 MiB of HBM per device.

```python
import math
import jax
import jax.numpy as jnp
from jax import lax

ROWS = 8192
KV = 1024
LAYERS_ALL = 4
PARTIALS = 8


def draw_grad_parts(key, part):
    subkeys = jax.random.split(key, 5)
    full_shape = (LAYERS_ALL, PARTIALS, ROWS, KV)
    col_scale = jnp.exp(jax.random.uniform(subkeys[0], (LAYERS_ALL, 1, 1, KV), jnp.float32, math.log(0.2), math.log(5.0)))
    row_scale = jnp.exp(jax.random.uniform(subkeys[1], (LAYERS_ALL, 1, ROWS, 1), jnp.float32, math.log(0.5), math.log(2.0)))
    owner_block = jax.random.randint(subkeys[2], (LAYERS_ALL, PARTIALS, 1, 1), 0, PARTIALS)
    row_block = (jnp.arange(ROWS, dtype=jnp.int32) // (ROWS // PARTIALS)).reshape(1, 1, ROWS, 1)
    spike_gain = jnp.where(row_block == owner_block, 4.0, 1.0)
    basis_values = jnp.clip(jax.random.normal(subkeys[3], full_shape, jnp.float32), -6.0, 6.0)
    return (basis_values * col_scale * row_scale * spike_gain).astype(jnp.bfloat16)


def plant(result, key, least, high):
    longest = result.shape.index(max(result.shape))
    spots = []
    for shift in (0, 1):
        where = [jax.random.randint(jax.random.fold_in(key, axis), (), 0, length) for axis, length in enumerate(result.shape)]
        where[longest] = (where[longest] + shift) % result.shape[longest]
        spots.append(tuple(where))
    return result.at[spots[0]].set(least).at[spots[1]].set(high)


def shard_levels(rng, extent, cuts, least, largest):
    factor_of = 1.0
    for position, shards_of in cuts:
        heights = jax.random.uniform(jax.random.fold_in(jax.random.fold_in(rng, 6), position), (shards_of,), jnp.float32, least / len(cuts), largest / len(cuts))
        factor_of = factor_of * jnp.repeat(jnp.exp(heights), extent[position] // shards_of).reshape((-1,) + (1,) * (len(extent) - 1 - position))
    return factor_of


def setup_inputs(seed: int = 0) -> dict:
    keys = jax.random.split(jax.random.key(seed), 8)
    return {
        "grad_parts": draw_grad_parts(jax.random.fold_in(keys[7], 71), 0),
        "first_codes": plant(jax.random.randint(keys[1], (LAYERS_ALL, ROWS, KV), -7, 8), jax.random.fold_in(keys[1], 1), -7, 7).astype(jnp.int32),
        "first_rows": jnp.clip(jnp.exp(math.log(0.03) - 2.3025851 * jax.random.uniform(keys[2], (LAYERS_ALL, ROWS), jnp.float32) ** shard_levels(keys[2], (LAYERS_ALL, ROWS), ((0, 4), (1, 8)), -0.2, 0.2)), 0.003, 0.03),
        "first_columns": jnp.clip(jnp.exp(math.log(0.03) - 2.3025851 * jax.random.uniform(keys[3], (LAYERS_ALL, KV), jnp.float32) ** shard_levels(keys[3], (LAYERS_ALL, KV), ((0, 4),), -0.2, 0.2)), 0.003, 0.03),
        "second_codes": plant(jax.random.randint(keys[4], (LAYERS_ALL, ROWS, KV), 1, 16), jax.random.fold_in(keys[4], 1), 1, 15).astype(jnp.int32),
        "second_rows": jnp.clip(jnp.exp(math.log(0.01) - 2.30258502 * jax.random.uniform(keys[5], (LAYERS_ALL, ROWS), jnp.float32) ** shard_levels(keys[5], (LAYERS_ALL, ROWS), ((0, 4), (1, 8)), -0.2, 0.2)), 0.001, 0.01),
        "second_columns": jnp.clip(jnp.exp(math.log(0.01) - 2.30258502 * jax.random.uniform(keys[6], (LAYERS_ALL, KV), jnp.float32) ** shard_levels(keys[6], (LAYERS_ALL, KV), ((0, 4),), -0.2, 0.2)), 0.001, 0.01),
    }


beta_first = 0.9
beta_second = 0.999
clip_rms = 3.0
epsilon = 1e-08
scale_floor = 0.001

def dequantize(code_values, levels, row_scale, col_scale):
    scale_bound = jnp.minimum(row_scale[:, :, None], col_scale[:, None, :])
    return code_values.astype(jnp.float32) / levels * scale_bound

def moments(gradient, clip_scale, first_codes, first_rows, first_columns, second_codes, second_rows, second_columns):
    first_old = dequantize(first_codes, 7.0, first_rows, first_columns)
    second_old = dequantize(second_codes, 15.0, second_rows, second_columns)
    clipped = clip_scale * gradient
    first_new = beta_first * first_old + (1.0 - beta_first) * clipped
    second_new = beta_second * second_old + (1.0 - beta_second) * clipped * clipped
    direction = first_new / (jnp.sqrt(second_new) + epsilon)
    return (first_new, second_new, direction)

def reference(grad_parts, first_codes, first_rows, first_columns, second_codes, second_rows, second_columns):

    def add_part(which_part, running):
        partial_value = lax.dynamic_index_in_dim(grad_parts, which_part, 1, keepdims=False)
        return running + partial_value.astype(jnp.float32)
    gradient = lax.fori_loop(0, PARTIALS, add_part, jnp.zeros((LAYERS_ALL, ROWS, KV), jnp.float32))
    square_sum = jnp.sum(gradient * gradient)
    clip_limit = clip_rms * math.sqrt(LAYERS_ALL * ROWS * KV)
    clip_scale = clip_limit / jnp.maximum(jnp.sqrt(square_sum), clip_limit)
    first_new, second_new, direction = moments(gradient, clip_scale, first_codes, first_rows, first_columns, second_codes, second_rows, second_columns)
    first_rowmax = jnp.maximum(lax.optimization_barrier(jnp.max(jnp.abs(first_new), axis=2)), scale_floor)
    first_colmax = jnp.maximum(lax.optimization_barrier(jnp.max(jnp.abs(first_new), axis=1)), scale_floor)
    second_rowmax = lax.optimization_barrier(jnp.max(second_new, axis=2))
    second_colmax = lax.optimization_barrier(jnp.max(second_new, axis=1))
    first_scaled = first_new / jnp.minimum(first_rowmax[:, :, None], first_colmax[:, None, :])
    second_scaled = second_new / jnp.minimum(second_rowmax[:, :, None], second_colmax[:, None, :])
    return (direction, first_scaled, second_scaled, first_rowmax, first_colmax, second_rowmax, second_colmax)
```

```python
import functools
import math

import jax
import jax.numpy as jnp
from jax import lax
from jax.experimental import pallas as pl
from jax.experimental.pallas import tpu as pltpu
from jax.sharding import PartitionSpec as P

beta_first = 0.9
beta_second = 0.999
clip_rms = 3.0
epsilon = 1e-08
scale_floor = 0.001

CORES = 2
SLAB = 128
LANES = 128
LAG = 2
PIECE = 16
LEVELS = 32767.0
TINY = 1e-37
VMEM_BYTES = 67043328
F32 = jnp.float32


def exchange_kernel(
    chips,
    fsdp,
    sections,
    slabs,
    clip_limit,
    grads,
    first_codes,
    first_rows,
    first_cols,
    second_codes,
    second_rows,
    second_cols,
    first_out,
    second_out,
    first_colmax,
    second_colmax,
    own,
    part,
    right_code,
    left_code,
    right_top,
    left_top,
    stage,
    total,
    codes_a,
    codes_b,
    first,
    second,
    square_send,
    square_recv,
    cross_send,
    cross_recv,
    col_send,
    col_recv,
    own_sem,
    part_send_sem,
    part_recv_sem,
    right_sems,
    left_sems,
    code_sem,
    out_sem,
    square_sems,
    cross_sems,
    col_sems,
):
    me = lax.axis_index("fsdp")
    section = lax.axis_index("section")
    chip = me // CORES
    core = me % CORES
    partner = chip * CORES + (1 - core)
    right = ((chip + 1) % chips) * CORES + core
    left = ((chip + chips - 1) % chips) * CORES + core
    cols = total.shape[-1]
    items = (chips - 1) * slabs

    def own_copy(dest, slab):
        return pltpu.make_async_copy(
            grads.at[dest, core, slab], own.at[dest, slab], own_sem.at[dest * slabs + slab]
        )

    def part_copy(dest, slab):
        return pltpu.make_async_remote_copy(
            src_ref=grads.at[dest, 1 - core, slab],
            dst_ref=part.at[dest, slab],
            send_sem=part_send_sem.at[dest * slabs + slab],
            recv_sem=part_recv_sem.at[dest * slabs + slab],
            device_id={"fsdp": partner},
            device_id_type=pl.DeviceIdType.MESH,
        )

    def hop(wire, tops, sems, slot, target):
        return tuple(
            pltpu.make_async_remote_copy(
                src_ref=ref.at[slot],
                dst_ref=ref.at[slot],
                send_sem=sems.at[2 * kind, slot],
                recv_sem=sems.at[2 * kind + 1, slot],
                device_id={"fsdp": target},
                device_id_type=pl.DeviceIdType.MESH,
            )
            for kind, ref in enumerate((wire, tops))
        )

    def right_slot(dest, slab):
        return (dest - 1) * slabs + slab

    def left_slot(dest, slab):
        return dest * slabs + slab

    def right_hop(slot):
        return hop(right_code, right_top, right_sems, slot, right)

    def left_hop(slot):
        return hop(left_code, left_top, left_sems, slot, left)

    def start(copies):
        for copy in copies:
            copy.start()

    def wait_recv(copies):
        for copy in copies:
            copy.wait_recv()

    def piece_rows(i):
        return pl.ds(pl.multiple_of(i * PIECE, PIECE), PIECE)

    def encode(term, wire, tops, slot):
        def collect(i, high):
            rows = piece_rows(i)
            value = term(rows)
            stage[rows, :] = value
            return jnp.maximum(
                high, jnp.max(jnp.abs(value).reshape(PIECE // 8, 8, cols), axis=0)
            )

        high = lax.fori_loop(0, SLAB // PIECE, collect, jnp.zeros((8, cols), F32))
        top = jnp.maximum(jnp.max(high, axis=0, keepdims=True), TINY)
        tops[slot] = top
        gain = LEVELS * lax.rsqrt(top)

        @pl.loop(0, SLAB // PIECE)
        def _(i):
            rows = piece_rows(i)
            value = stage[rows, :]
            root = value * lax.rsqrt(jnp.maximum(jnp.abs(value), TINY))
            wire[slot, rows, :] = jnp.round(root * gain).astype(jnp.int32).astype(jnp.int16)

    def decoder(wire, tops, slot):
        unit = tops[slot] * (1.0 / (LEVELS * LEVELS))

        def decode(rows):
            code = wire[slot, rows, :].astype(jnp.int32).astype(F32)
            return code * jnp.abs(code) * unit

        return decode

    def add_total(slab, decode):
        @pl.loop(0, SLAB // PIECE)
        def _(i):
            rows = piece_rows(i)
            total[slab, rows, :] += decode(rows)

    def wait_pair(dest, slab):
        own_copy(dest, slab).wait()
        part_copy(dest, slab).wait_recv()

    def pair_sum(dest, slab):
        def term(rows):
            return own[dest, slab, rows, :].astype(F32) + part[dest, slab, rows, :].astype(F32)

        return term

    def joined(decode, pair):
        return lambda rows: decode(rows) + pair(rows)

    @pl.loop(0, chips * slabs)
    def _(i):
        step, slab = i // slabs, i % slabs
        dest = jnp.where(2 * chip < chips, chips - 1 - step, step)
        own_copy(dest, slab).start()
        part_copy(dest, slab).start()

    code_copies = (
        pltpu.make_async_copy(first_codes, codes_a, code_sem.at[0]),
        pltpu.make_async_copy(second_codes, codes_b, code_sem.at[1]),
    )
    for copy in code_copies:
        copy.start()

    @pl.when(chip == 0)
    def _():
        @pl.loop(0, items)
        def _(j):
            dest, slab = chips - 1 - j // slabs, j % slabs
            wait_pair(dest, slab)
            slot = right_slot(dest, slab)
            encode(pair_sum(dest, slab), right_code, right_top, slot)
            start(right_hop(slot))

    @pl.when(chip == chips - 1)
    def _():
        @pl.loop(0, items)
        def _(j):
            dest, slab = j // slabs, j % slabs
            wait_pair(dest, slab)
            slot = left_slot(dest, slab)
            encode(pair_sum(dest, slab), left_code, left_top, slot)
            start(left_hop(slot))

    @pl.loop(0, slabs)
    def _(slab):
        wait_pair(chip, slab)
        term = pair_sum(chip, slab)

        @pl.loop(0, SLAB // PIECE)
        def _(i):
            rows = piece_rows(i)
            total[slab, rows, :] = term(rows)

    for copy in code_copies:
        copy.wait()

    @pl.loop(0, slabs)
    def _(slab):
        rows = pl.ds(pl.multiple_of(slab * SLAB, SLAB), SLAB)
        first_row = jnp.broadcast_to(first_rows[:, rows], (LANES, SLAB)).T
        second_row = jnp.broadcast_to(second_rows[:, rows], (LANES, SLAB)).T
        for q in range(cols // LANES):
            span = pl.ds(q * LANES, LANES)
            first_bound = jnp.minimum(first_row, first_cols[:, span])
            second_bound = jnp.minimum(second_row, second_cols[:, span])
            first_old = codes_a[slab, :, span].astype(F32) / 7.0 * first_bound
            second_old = codes_b[slab, :, span].astype(F32) / 15.0 * second_bound
            first[slab, :, span] = beta_first * first_old
            second[slab, :, span] = beta_second * second_old

    right_lag = LAG * chip
    left_lag = LAG * (chips - 1 - chip)

    @pl.loop(0, items + LAG * (chips - 1))
    def _(step):
        j = step - right_lag
        dest = chips - 1 - j // slabs
        slab = j % slabs

        @pl.when((chip > 0) & (j >= 0) & (dest >= chip))
        def _():
            slot = right_slot(dest, slab)
            wait_recv(right_hop(slot))
            decode = decoder(right_code, right_top, slot)

            @pl.when(dest > chip)
            def _():
                wait_pair(dest, slab)
                encode(joined(decode, pair_sum(dest, slab)), right_code, right_top, slot)
                start(right_hop(slot))

            @pl.when(dest == chip)
            def _():
                add_total(slab, decode)

        i = step - left_lag
        low = i // slabs
        strip = i % slabs

        @pl.when((chip < chips - 1) & (i >= 0) & (low <= chip))
        def _():
            slot = left_slot(low, strip)
            wait_recv(left_hop(slot))
            decode = decoder(left_code, left_top, slot)

            @pl.when(low < chip)
            def _():
                wait_pair(low, strip)
                encode(joined(decode, pair_sum(low, strip)), left_code, left_top, slot)
                start(left_hop(slot))

            @pl.when(low == chip)
            def _():
                add_total(strip, decode)

    piece = 16
    pieces = SLAB // piece

    def add_squares(i, acc):
        slab, rows = i // pieces, pl.ds(pl.multiple_of((i % pieces) * piece, piece), piece)
        g = total[slab, rows, :]
        return acc + jnp.sum((g * g).reshape(piece // 8, 8, cols), axis=0)

    squares = lax.fori_loop(0, slabs * pieces, add_squares, jnp.zeros((8, cols), F32))
    folded = squares[:, :LANES]
    for q in range(1, cols // LANES):
        folded = folded + squares[:, q * LANES : (q + 1) * LANES]

    def to_all(axis, size, position, source, slots, sems):
        copies = [
            pltpu.make_async_remote_copy(
                src_ref=source,
                dst_ref=slots.at[s - 1],
                send_sem=sems.at[0, s - 1],
                recv_sem=sems.at[1, s - 1],
                device_id={axis: (position + s) % size},
                device_id_type=pl.DeviceIdType.MESH,
            )
            for s in range(1, size)
        ]
        for copy in copies:
            copy.start()
        return copies

    square_send[...] = folded
    square_copies = to_all("fsdp", fsdp, me, square_send, square_recv, square_sems)
    for s, copy in enumerate(square_copies):
        copy.wait_recv()
        folded = folded + square_recv[s]
    cross_send[...] = folded
    cross_copies = to_all("section", sections, section, cross_send, cross_recv, cross_sems)
    for s, copy in enumerate(cross_copies):
        copy.wait_recv()
        folded = folded + cross_recv[s]
    square_sum = jnp.sum(jnp.sum(folded, axis=0, keepdims=True), axis=1, keepdims=True)
    norm = jnp.sqrt(jnp.broadcast_to(square_sum, (1, cols)))
    scale = clip_limit / jnp.maximum(norm, clip_limit)

    def out_copies(slab):
        return (
            pltpu.make_async_copy(first.at[slab], first_out.at[slab], out_sem.at[0, slab]),
            pltpu.make_async_copy(second.at[slab], second_out.at[slab], out_sem.at[1, slab]),
        )

    def update_slab(slab, carry):
        def update_piece(i, carry):
            first_top, second_top = carry
            rows = pl.ds(pl.multiple_of(i * piece, piece), piece)
            clipped = scale * total[slab, rows, :]
            first_new = first[slab, rows, :] + (1.0 - beta_first) * clipped
            second_new = second[slab, rows, :] + (1.0 - beta_second) * clipped * clipped
            first[slab, rows, :] = first_new
            second[slab, rows, :] = second_new
            high = jnp.max(jnp.abs(first_new).reshape(piece // 8, 8, cols), axis=0)
            top = jnp.max(second_new.reshape(piece // 8, 8, cols), axis=0)
            return jnp.maximum(first_top, high), jnp.maximum(second_top, top)

        carry = lax.fori_loop(0, pieces, update_piece, carry)
        for copy in out_copies(slab):
            copy.start()
        return carry

    nothing = jnp.zeros((8, cols), F32)
    first_top, second_top = lax.fori_loop(0, slabs, update_slab, (nothing, nothing))
    first_top = jnp.max(first_top, axis=0, keepdims=True)
    second_top = jnp.max(second_top, axis=0, keepdims=True)
    col_send[0:1, :] = first_top
    col_send[1:2, :] = second_top
    col_copies = to_all("fsdp", fsdp, me, col_send, col_recv, col_sems)

    @pl.loop(0, chips * slabs)
    def _(i):
        part_copy(i // slabs, i % slabs).wait_send()

    @pl.loop(0, items)
    def _(j):
        slab = j % slabs

        @pl.when(j // slabs + 1 > chip)
        def _():
            for copy in right_hop(right_slot(j // slabs + 1, slab)):
                copy.wait_send()

        @pl.when(j // slabs < chip)
        def _():
            for copy in left_hop(left_slot(j // slabs, slab)):
                copy.wait_send()

    for copy in square_copies + cross_copies:
        copy.wait_send()

    for s, copy in enumerate(col_copies):
        copy.wait_recv()
        first_top = jnp.maximum(first_top, col_recv[s, 0:1, :])
        second_top = jnp.maximum(second_top, col_recv[s, 1:2, :])
    first_colmax[...] = jnp.maximum(first_top, scale_floor)
    second_colmax[...] = second_top
    for copy in col_copies:
        copy.wait_send()

    @pl.loop(0, slabs)
    def _(slab):
        for copy in out_copies(slab):
            copy.wait()


def finish_kernel(
    first,
    second,
    first_colmax,
    second_colmax,
    direction,
    first_scaled,
    second_scaled,
    first_rowmax,
    second_rowmax,
    first_kept,
    second_kept,
):
    first_new = first[0]
    second_new = second[0]
    first_top = jnp.maximum(jnp.max(jnp.abs(first_new), axis=1, keepdims=True), scale_floor)
    second_top = jnp.max(second_new, axis=1, keepdims=True)
    direction[0] = first_new / (jnp.sqrt(second_new) + epsilon)
    first_scaled[0] = first_new / jnp.minimum(first_top, first_colmax[...])
    second_scaled[0] = second_new / jnp.minimum(second_top, second_colmax[...])
    first_rowmax[...] = jnp.broadcast_to(first_top, (SLAB, LANES)).T[0:1, :]
    second_rowmax[...] = jnp.broadcast_to(second_top, (SLAB, LANES)).T[0:1, :]
    first_kept[...] = first_colmax[...]
    second_kept[...] = second_colmax[...]


def local(
    grad_parts, first_codes, first_rows, first_columns, second_codes, second_rows, second_columns
):
    fsdp = lax.axis_size("fsdp")
    sections = lax.axis_size("section")
    layers, _, row_count, cols = grad_parts.shape
    chips = fsdp // CORES
    rows = row_count // fsdp
    slabs = rows // SLAB
    clip_limit = clip_rms * math.sqrt(layers * sections * row_count * cols)
    grads = grad_parts.reshape(chips, CORES, slabs, SLAB, cols)
    tiled = (slabs, SLAB, cols)
    items = (chips - 1) * slabs
    hbm = pl.BlockSpec(memory_space=pl.ANY)
    vmem = pl.BlockSpec(memory_space=pltpu.VMEM)
    dma = pltpu.SemaphoreType.DMA
    first_new, second_new, first_colmax, second_colmax = pl.pallas_call(
        functools.partial(exchange_kernel, chips, fsdp, sections, slabs, clip_limit),
        out_shape=(
            jax.ShapeDtypeStruct(tiled, F32),
            jax.ShapeDtypeStruct(tiled, F32),
            jax.ShapeDtypeStruct((1, cols), F32),
            jax.ShapeDtypeStruct((1, cols), F32),
        ),
        in_specs=[hbm, hbm, vmem, vmem, hbm, vmem, vmem],
        out_specs=(hbm, hbm, vmem, vmem),
        scratch_shapes=[
            pltpu.VMEM((chips, *tiled), jnp.bfloat16),
            pltpu.VMEM((chips, *tiled), jnp.bfloat16),
            pltpu.VMEM((items, SLAB, cols), jnp.int16),
            pltpu.VMEM((items, SLAB, cols), jnp.int16),
            pltpu.VMEM((items, 1, cols), F32),
            pltpu.VMEM((items, 1, cols), F32),
            pltpu.VMEM((SLAB, cols), F32),
            pltpu.VMEM(tiled, F32),
            pltpu.VMEM(tiled, jnp.int32),
            pltpu.VMEM(tiled, jnp.int32),
            pltpu.VMEM(tiled, F32),
            pltpu.VMEM(tiled, F32),
            pltpu.VMEM((8, LANES), F32),
            pltpu.VMEM((fsdp - 1, 8, LANES), F32),
            pltpu.VMEM((8, LANES), F32),
            pltpu.VMEM((max(sections - 1, 1), 8, LANES), F32),
            pltpu.VMEM((2, cols), F32),
            pltpu.VMEM((fsdp - 1, 2, cols), F32),
            dma((chips * slabs,)),
            dma((chips * slabs,)),
            dma((chips * slabs,)),
            dma((4, items)),
            dma((4, items)),
            dma((2,)),
            dma((2, slabs)),
            dma((2, fsdp - 1)),
            dma((2, max(sections - 1, 1))),
            dma((2, fsdp - 1)),
        ],
        compiler_params=pltpu.CompilerParams(
            has_side_effects=True, vmem_limit_bytes=VMEM_BYTES
        ),
    )(
        grads,
        first_codes.reshape(tiled),
        first_rows,
        first_columns,
        second_codes.reshape(tiled),
        second_rows,
        second_columns,
    )
    block = pl.BlockSpec((1, SLAB, cols), lambda i: (i, 0, 0))
    whole = pl.BlockSpec((1, cols), lambda i: (0, 0))
    strip = pl.BlockSpec((1, SLAB), lambda i: (0, i))
    finished = pl.pallas_call(
        finish_kernel,
        grid=(slabs,),
        out_shape=(
            jax.ShapeDtypeStruct(tiled, F32),
            jax.ShapeDtypeStruct(tiled, F32),
            jax.ShapeDtypeStruct(tiled, F32),
            jax.ShapeDtypeStruct((1, rows), F32),
            jax.ShapeDtypeStruct((1, rows), F32),
            jax.ShapeDtypeStruct((1, cols), F32),
            jax.ShapeDtypeStruct((1, cols), F32),
        ),
        in_specs=[block, block, whole, whole],
        out_specs=(block, block, block, strip, strip, whole, whole),
    )(first_new, second_new, first_colmax, second_colmax)
    direction, first_scaled, second_scaled = finished[:3]
    first_rowmax, second_rowmax, first_colmax, second_colmax = finished[3:]
    shape = (layers, rows, cols)
    return (
        direction.reshape(shape),
        first_scaled.reshape(shape),
        second_scaled.reshape(shape),
        first_rowmax,
        first_colmax,
        second_rowmax,
        second_colmax,
    )


def solution(mesh):
    placed = (
        P("section", "fsdp", None, None),
        P("section", "fsdp", None),
        P("section", "fsdp"),
        P("section", None),
        P("section", "fsdp", None),
        P("section", "fsdp"),
        P("section", None),
    )
    return jax.shard_map(
        local,
        mesh=mesh,
        in_specs=placed,
        out_specs=(
            P("section", "fsdp", None),
            P("section", "fsdp", None),
            P("section", "fsdp", None),
            P("section", "fsdp"),
            P("section", None),
            P("section", "fsdp"),
            P("section", None),
        ),
        check_vma=False,
    )
```

```python
import functools
import math

import jax
import jax.numpy as jnp
from jax import lax
from jax.experimental import pallas as pl
from jax.experimental.pallas import tpu as pltpu
from jax.sharding import PartitionSpec as P

beta_first = 0.9
beta_second = 0.999
clip_rms = 3.0
epsilon = 1e-08
scale_floor = 0.001

CORES = 2
SLAB = 128
LANES = 128
LAG = 2
PIECE = 16
LEVELS = 32767.0
TINY = 1e-37
EXCHANGE_VMEM = 44 * 2**20
FINISH_VMEM = 10 * 2**20
F32 = jnp.float32


def exchange_kernel(
    chips,
    fsdp,
    sections,
    slabs,
    clip_limit,
    grads,
    first_codes,
    first_rows,
    first_cols,
    second_codes,
    second_rows,
    second_cols,
    direction,
    first,
    second,
    first_inverse,
    second_inverse,
    first_rowmax,
    second_rowmax,
    first_colmax,
    second_colmax,
    own,
    part,
    right_code,
    left_code,
    right_top,
    left_top,
    stage,
    total,
    codes_a,
    codes_b,
    first_peak,
    second_peak,
    square_send,
    square_recv,
    cross_send,
    cross_recv,
    col_send,
    col_recv,
    own_sem,
    part_send_sem,
    part_recv_sem,
    right_sems,
    left_sems,
    code_sem,
    square_sems,
    cross_sems,
    col_sems,
):
    me = lax.axis_index("fsdp")
    section = lax.axis_index("section")
    chip = me // CORES
    core = me % CORES
    partner = chip * CORES + (1 - core)
    right = ((chip + 1) % chips) * CORES + core
    left = ((chip + chips - 1) % chips) * CORES + core
    cols = total.shape[-1]
    items = (chips - 1) * slabs

    def own_copy(dest, slab):
        return pltpu.make_async_copy(
            grads.at[dest, core, slab], own.at[dest, slab], own_sem.at[dest * slabs + slab]
        )

    def part_copy(dest, slab):
        return pltpu.make_async_remote_copy(
            src_ref=grads.at[dest, 1 - core, slab],
            dst_ref=part.at[dest, slab],
            send_sem=part_send_sem.at[dest * slabs + slab],
            recv_sem=part_recv_sem.at[dest * slabs + slab],
            device_id={"fsdp": partner},
            device_id_type=pl.DeviceIdType.MESH,
        )

    def hop(wire, tops, sems, slot, target):
        return tuple(
            pltpu.make_async_remote_copy(
                src_ref=ref.at[slot],
                dst_ref=ref.at[slot],
                send_sem=sems.at[2 * kind, slot],
                recv_sem=sems.at[2 * kind + 1, slot],
                device_id={"fsdp": target},
                device_id_type=pl.DeviceIdType.MESH,
            )
            for kind, ref in enumerate((wire, tops))
        )

    def right_slot(dest, slab):
        return (dest - 1) * slabs + slab

    def left_slot(dest, slab):
        return dest * slabs + slab

    def right_hop(slot):
        return hop(right_code, right_top, right_sems, slot, right)

    def left_hop(slot):
        return hop(left_code, left_top, left_sems, slot, left)

    def start(copies):
        for copy in copies:
            copy.start()

    def wait_recv(copies):
        for copy in copies:
            copy.wait_recv()

    def piece_rows(i):
        return pl.ds(pl.multiple_of(i * PIECE, PIECE), PIECE)

    def encode(term, wire, tops, slot):
        def collect(i, high):
            rows = piece_rows(i)
            value = term(rows)
            stage[rows, :] = value
            return jnp.maximum(
                high, jnp.max(jnp.abs(value).reshape(PIECE // 8, 8, cols), axis=0)
            )

        high = lax.fori_loop(0, SLAB // PIECE, collect, jnp.zeros((8, cols), F32))
        top = jnp.maximum(jnp.max(high, axis=0, keepdims=True), TINY)
        tops[slot] = top
        gain = LEVELS * lax.rsqrt(top)

        @pl.loop(0, SLAB // PIECE)
        def _(i):
            rows = piece_rows(i)
            value = stage[rows, :]
            root = value * lax.rsqrt(jnp.maximum(jnp.abs(value), TINY))
            wire[slot, rows, :] = jnp.round(root * gain).astype(jnp.int32).astype(jnp.int16)

    def decoder(wire, tops, slot):
        unit = tops[slot] * (1.0 / (LEVELS * LEVELS))

        def decode(rows):
            code = wire[slot, rows, :].astype(jnp.int32).astype(F32)
            return code * jnp.abs(code) * unit

        return decode

    def add_total(slab, decode):
        @pl.loop(0, SLAB // PIECE)
        def _(i):
            rows = piece_rows(i)
            total[slab, rows, :] += decode(rows)

    def wait_pair(dest, slab):
        own_copy(dest, slab).wait()
        part_copy(dest, slab).wait_recv()

    def pair_sum(dest, slab):
        def term(rows):
            return own[dest, slab, rows, :].astype(F32) + part[dest, slab, rows, :].astype(F32)

        return term

    def joined(decode, pair):
        return lambda rows: decode(rows) + pair(rows)

    @pl.loop(0, chips * slabs)
    def _(i):
        step, slab = i // slabs, i % slabs
        dest = jnp.where(2 * chip < chips, chips - 1 - step, step)
        own_copy(dest, slab).start()
        part_copy(dest, slab).start()

    code_copies = (
        pltpu.make_async_copy(first_codes, codes_a, code_sem.at[0]),
        pltpu.make_async_copy(second_codes, codes_b, code_sem.at[1]),
    )
    for copy in code_copies:
        copy.start()

    @pl.when(chip == 0)
    def _():
        @pl.loop(0, items)
        def _(j):
            dest, slab = chips - 1 - j // slabs, j % slabs
            wait_pair(dest, slab)
            slot = right_slot(dest, slab)
            encode(pair_sum(dest, slab), right_code, right_top, slot)
            start(right_hop(slot))

    @pl.when(chip == chips - 1)
    def _():
        @pl.loop(0, items)
        def _(j):
            dest, slab = j // slabs, j % slabs
            wait_pair(dest, slab)
            slot = left_slot(dest, slab)
            encode(pair_sum(dest, slab), left_code, left_top, slot)
            start(left_hop(slot))

    @pl.loop(0, slabs)
    def _(slab):
        wait_pair(chip, slab)
        term = pair_sum(chip, slab)

        @pl.loop(0, SLAB // PIECE)
        def _(i):
            rows = piece_rows(i)
            total[slab, rows, :] = term(rows)

    for copy in code_copies:
        copy.wait()

    @pl.loop(0, slabs)
    def _(slab):
        rows = pl.ds(pl.multiple_of(slab * SLAB, SLAB), SLAB)
        first_row = jnp.broadcast_to(first_rows[:, rows], (LANES, SLAB)).T
        second_row = jnp.broadcast_to(second_rows[:, rows], (LANES, SLAB)).T
        for q in range(cols // LANES):
            span = pl.ds(q * LANES, LANES)
            first_bound = jnp.minimum(first_row, first_cols[:, span])
            second_bound = jnp.minimum(second_row, second_cols[:, span])
            first_old = codes_a[slab, :, span].astype(F32) / 7.0 * first_bound
            second_old = codes_b[slab, :, span].astype(F32) / 15.0 * second_bound
            first[slab, :, span] = beta_first * first_old
            second[slab, :, span] = beta_second * second_old

    right_lag = LAG * chip
    left_lag = LAG * (chips - 1 - chip)

    @pl.loop(0, items + LAG * (chips - 1))
    def _(step):
        j = step - right_lag
        dest = chips - 1 - j // slabs
        slab = j % slabs

        @pl.when((chip > 0) & (j >= 0) & (dest >= chip))
        def _():
            slot = right_slot(dest, slab)
            wait_recv(right_hop(slot))
            decode = decoder(right_code, right_top, slot)

            @pl.when(dest > chip)
            def _():
                wait_pair(dest, slab)
                encode(joined(decode, pair_sum(dest, slab)), right_code, right_top, slot)
                start(right_hop(slot))

            @pl.when(dest == chip)
            def _():
                add_total(slab, decode)

        i = step - left_lag
        low = i // slabs
        strip = i % slabs

        @pl.when((chip < chips - 1) & (i >= 0) & (low <= chip))
        def _():
            slot = left_slot(low, strip)
            wait_recv(left_hop(slot))
            decode = decoder(left_code, left_top, slot)

            @pl.when(low < chip)
            def _():
                wait_pair(low, strip)
                encode(joined(decode, pair_sum(low, strip)), left_code, left_top, slot)
                start(left_hop(slot))

            @pl.when(low == chip)
            def _():
                add_total(strip, decode)

    piece = 16
    pieces = SLAB // piece

    def add_squares(i, acc):
        slab, rows = i // pieces, pl.ds(pl.multiple_of((i % pieces) * piece, piece), piece)
        g = total[slab, rows, :]
        return acc + jnp.sum((g * g).reshape(piece // 8, 8, cols), axis=0)

    squares = lax.fori_loop(0, slabs * pieces, add_squares, jnp.zeros((8, cols), F32))
    folded = squares[:, :LANES]
    for q in range(1, cols // LANES):
        folded = folded + squares[:, q * LANES : (q + 1) * LANES]

    def to_all(axis, size, position, source, slots, sems):
        copies = [
            pltpu.make_async_remote_copy(
                src_ref=source,
                dst_ref=slots.at[s - 1],
                send_sem=sems.at[0, s - 1],
                recv_sem=sems.at[1, s - 1],
                device_id={axis: (position + s) % size},
                device_id_type=pl.DeviceIdType.MESH,
            )
            for s in range(1, size)
        ]
        for copy in copies:
            copy.start()
        return copies

    square_send[...] = folded
    square_copies = to_all("fsdp", fsdp, me, square_send, square_recv, square_sems)
    for s, copy in enumerate(square_copies):
        copy.wait_recv()
        folded = folded + square_recv[s]
    cross_send[...] = folded
    cross_copies = to_all("section", sections, section, cross_send, cross_recv, cross_sems)
    for s, copy in enumerate(cross_copies):
        copy.wait_recv()
        folded = folded + cross_recv[s]
    square_sum = jnp.sum(jnp.sum(folded, axis=0, keepdims=True), axis=1, keepdims=True)
    norm = jnp.sqrt(jnp.broadcast_to(square_sum, (1, cols)))
    scale = clip_limit / jnp.maximum(norm, clip_limit)

    def update_piece(i, carry):
        first_top, second_top = carry
        slab, rows = i // pieces, piece_rows(i % pieces)
        clipped = scale * total[slab, rows, :]
        first_new = first[slab, rows, :] + (1.0 - beta_first) * clipped
        second_new = second[slab, rows, :] + (1.0 - beta_second) * clipped * clipped
        first[slab, rows, :] = first_new
        second[slab, rows, :] = second_new
        high = jnp.max(jnp.abs(first_new).reshape(piece // 8, 8, cols), axis=0)
        top = jnp.max(second_new.reshape(piece // 8, 8, cols), axis=0)
        return jnp.maximum(first_top, high), jnp.maximum(second_top, top)

    nothing = jnp.zeros((8, cols), F32)
    first_top, second_top = lax.fori_loop(
        0, slabs * pieces, update_piece, (nothing, nothing)
    )
    first_top = jnp.max(first_top, axis=0, keepdims=True)
    second_top = jnp.max(second_top, axis=0, keepdims=True)
    col_send[0:1, :] = first_top
    col_send[1:2, :] = second_top
    col_copies = to_all("fsdp", fsdp, me, col_send, col_recv, col_sems)

    def lane_peak(block):
        peak = block[:, :LANES]
        for q in range(1, cols // LANES):
            peak = jnp.maximum(peak, block[:, q * LANES : (q + 1) * LANES])
        return peak

    @pl.loop(0, slabs)
    def _(slab):
        @pl.loop(0, pieces)
        def _(i):
            rows = piece_rows(i)
            first_new = first[slab, rows, :]
            second_new = second[slab, rows, :]
            direction[slab, rows, :] = first_new / (jnp.sqrt(second_new) + epsilon)
            first_peak[rows, :] = lane_peak(jnp.abs(first_new))
            second_peak[rows, :] = lane_peak(second_new)

        span = pl.ds(pl.multiple_of(slab * SLAB, SLAB), SLAB)
        first_row = jnp.max(first_peak[...], axis=1, keepdims=True)
        first_row = jnp.broadcast_to(jnp.maximum(first_row, scale_floor), (SLAB, LANES))
        second_row = jnp.max(second_peak[...], axis=1, keepdims=True)
        second_row = jnp.broadcast_to(second_row, (SLAB, LANES))
        first_inverse[slab] = 1.0 / first_row
        second_inverse[slab] = 1.0 / second_row
        first_rowmax[:, span] = first_row.T[0:1, :]
        second_rowmax[:, span] = second_row.T[0:1, :]

    @pl.loop(0, chips * slabs)
    def _(i):
        part_copy(i // slabs, i % slabs).wait_send()

    @pl.loop(0, items)
    def _(j):
        slab = j % slabs

        @pl.when(j // slabs + 1 > chip)
        def _():
            for copy in right_hop(right_slot(j // slabs + 1, slab)):
                copy.wait_send()

        @pl.when(j // slabs < chip)
        def _():
            for copy in left_hop(left_slot(j // slabs, slab)):
                copy.wait_send()

    for copy in square_copies + cross_copies:
        copy.wait_send()

    for s, copy in enumerate(col_copies):
        copy.wait_recv()
        first_top = jnp.maximum(first_top, col_recv[s, 0:1, :])
        second_top = jnp.maximum(second_top, col_recv[s, 1:2, :])
    first_colmax[...] = jnp.maximum(first_top, scale_floor)
    second_colmax[...] = second_top
    for copy in col_copies:
        copy.wait_send()


def finish_kernel(
    direction,
    first,
    second,
    first_inverse,
    second_inverse,
    first_rowmax,
    second_rowmax,
    first_colmax,
    second_colmax,
    direction_out,
    first_out,
    second_out,
    first_row_out,
    first_col_out,
    second_row_out,
    second_col_out,
    first_scaled,
    second_scaled,
    direction_sem,
    out_sem,
    small_sem,
):
    slabs, _, cols = first.shape
    small = (
        (first_rowmax, first_row_out),
        (first_colmax, first_col_out),
        (second_rowmax, second_row_out),
        (second_colmax, second_col_out),
    )
    copies = [
        pltpu.make_async_copy(direction.at[slab], direction_out.at[slab], direction_sem.at[slab])
        for slab in range(slabs)
    ]
    copies += [
        pltpu.make_async_copy(source, target, small_sem.at[i])
        for i, (source, target) in enumerate(small)
    ]
    for copy in copies:
        copy.start()
    first_col = 1.0 / first_colmax[...]
    second_col = 1.0 / second_colmax[...]

    def out_copies(slab):
        return (
            pltpu.make_async_copy(first_scaled.at[slab], first_out.at[slab], out_sem.at[0, slab]),
            pltpu.make_async_copy(
                second_scaled.at[slab], second_out.at[slab], out_sem.at[1, slab]
            ),
        )

    @pl.loop(0, slabs)
    def _(slab):
        @pl.loop(0, SLAB // PIECE)
        def _(i):
            rows = pl.ds(pl.multiple_of(i * PIECE, PIECE), PIECE)
            first_row = first_inverse[slab, rows, :]
            second_row = second_inverse[slab, rows, :]
            for q in range(cols // LANES):
                span = slice(q * LANES, (q + 1) * LANES)
                first_scaled[slab, rows, span] = first[slab, rows, span] * jnp.maximum(
                    first_row, first_col[:, span]
                )
                second_scaled[slab, rows, span] = second[slab, rows, span] * jnp.maximum(
                    second_row, second_col[:, span]
                )

        for copy in out_copies(slab):
            copy.start()

    for copy in copies:
        copy.wait()

    @pl.loop(0, slabs)
    def _(slab):
        for copy in out_copies(slab):
            copy.wait()


def local(
    grad_parts, first_codes, first_rows, first_columns, second_codes, second_rows, second_columns
):
    fsdp = lax.axis_size("fsdp")
    sections = lax.axis_size("section")
    layers, _, row_count, cols = grad_parts.shape
    chips = fsdp // CORES
    rows = row_count // fsdp
    slabs = rows // SLAB
    clip_limit = clip_rms * math.sqrt(layers * sections * row_count * cols)
    grads = grad_parts.reshape(chips, CORES, slabs, SLAB, cols)
    tiled = (slabs, SLAB, cols)
    items = (chips - 1) * slabs
    hbm = pl.BlockSpec(memory_space=pl.ANY)
    vmem = pl.BlockSpec(memory_space=pltpu.VMEM)
    dma = pltpu.SemaphoreType.DMA
    inverse = (slabs, SLAB, LANES)
    kept = (tiled, tiled, tiled, inverse, inverse, (1, rows), (1, rows), (1, cols), (1, cols))
    held = pl.pallas_call(
        functools.partial(exchange_kernel, chips, fsdp, sections, slabs, clip_limit),
        out_shape=tuple(pltpu.VMEM(shape, F32) for shape in kept),
        in_specs=[hbm, hbm, vmem, vmem, hbm, vmem, vmem],
        out_specs=(vmem,) * len(kept),
        scratch_shapes=[
            pltpu.VMEM((chips, *tiled), jnp.bfloat16),
            pltpu.VMEM((chips, *tiled), jnp.bfloat16),
            pltpu.VMEM((items, SLAB, cols), jnp.int16),
            pltpu.VMEM((items, SLAB, cols), jnp.int16),
            pltpu.VMEM((items, 1, cols), F32),
            pltpu.VMEM((items, 1, cols), F32),
            pltpu.VMEM((SLAB, cols), F32),
            pltpu.VMEM(tiled, F32),
            pltpu.VMEM(tiled, jnp.int32),
            pltpu.VMEM(tiled, jnp.int32),
            pltpu.VMEM((SLAB, LANES), F32),
            pltpu.VMEM((SLAB, LANES), F32),
            pltpu.VMEM((8, LANES), F32),
            pltpu.VMEM((fsdp - 1, 8, LANES), F32),
            pltpu.VMEM((8, LANES), F32),
            pltpu.VMEM((max(sections - 1, 1), 8, LANES), F32),
            pltpu.VMEM((2, cols), F32),
            pltpu.VMEM((fsdp - 1, 2, cols), F32),
            dma((chips * slabs,)),
            dma((chips * slabs,)),
            dma((chips * slabs,)),
            dma((4, items)),
            dma((4, items)),
            dma((2,)),
            dma((2, fsdp - 1)),
            dma((2, max(sections - 1, 1))),
            dma((2, fsdp - 1)),
        ],
        compiler_params=pltpu.CompilerParams(
            has_side_effects=True, vmem_limit_bytes=EXCHANGE_VMEM
        ),
    )(
        grads,
        first_codes.reshape(tiled),
        first_rows,
        first_columns,
        second_codes.reshape(tiled),
        second_rows,
        second_columns,
    )
    finished = pl.pallas_call(
        finish_kernel,
        out_shape=(
            jax.ShapeDtypeStruct(tiled, F32),
            jax.ShapeDtypeStruct(tiled, F32),
            jax.ShapeDtypeStruct(tiled, F32),
            jax.ShapeDtypeStruct((1, rows), F32),
            jax.ShapeDtypeStruct((1, cols), F32),
            jax.ShapeDtypeStruct((1, rows), F32),
            jax.ShapeDtypeStruct((1, cols), F32),
        ),
        in_specs=[vmem] * len(kept),
        out_specs=(hbm,) * 7,
        scratch_shapes=[
            pltpu.VMEM(tiled, F32),
            pltpu.VMEM(tiled, F32),
            dma((slabs,)),
            dma((2, slabs)),
            dma((4,)),
        ],
        compiler_params=pltpu.CompilerParams(vmem_limit_bytes=FINISH_VMEM),
    )(*(pltpu.with_memory_space_constraint(x, pltpu.VMEM) for x in held))
    direction, first_scaled, second_scaled = finished[:3]
    first_rowmax, first_colmax, second_rowmax, second_colmax = finished[3:]
    shape = (layers, rows, cols)
    return (
        direction.reshape(shape),
        first_scaled.reshape(shape),
        second_scaled.reshape(shape),
        first_rowmax,
        first_colmax,
        second_rowmax,
        second_colmax,
    )


def solution(mesh):
    placed = (
        P("section", "fsdp", None, None),
        P("section", "fsdp", None),
        P("section", "fsdp"),
        P("section", None),
        P("section", "fsdp", None),
        P("section", "fsdp"),
        P("section", None),
    )
    return jax.shard_map(
        local,
        mesh=mesh,
        in_specs=placed,
        out_specs=(
            P("section", "fsdp", None),
            P("section", "fsdp", None),
            P("section", "fsdp", None),
            P("section", "fsdp"),
            P("section", None),
            P("section", "fsdp"),
            P("section", None),
        ),
        check_vma=False,
    )
```

```python
import functools
import math

import jax
import jax.numpy as jnp
from jax import lax
from jax.experimental import pallas as pl
from jax.experimental.pallas import tpu as pltpu
from jax.sharding import PartitionSpec as P

beta_first = 0.9
beta_second = 0.999
clip_rms = 3.0
epsilon = 1e-08
scale_floor = 0.001

CORES = 2
SLAB = 128
LANES = 128
LAG = 2
PIECE = 16
UNROLL = 4
LEVELS = 32767.0
TINY = 1e-37
EXCHANGE_VMEM = 44 * 2**20
FINISH_VMEM = 10 * 2**20
F32 = jnp.float32


def exchange_kernel(
    chips,
    fsdp,
    sections,
    slabs,
    clip_limit,
    grads,
    first_codes,
    first_rows,
    first_cols,
    second_codes,
    second_rows,
    second_cols,
    direction,
    first,
    second,
    first_inverse,
    second_inverse,
    first_rowmax,
    second_rowmax,
    first_colmax,
    second_colmax,
    own,
    part,
    right_code,
    left_code,
    right_top,
    left_top,
    stage,
    total,
    codes_a,
    codes_b,
    first_peak,
    second_peak,
    square_send,
    square_recv,
    col_send,
    col_recv,
    own_sem,
    part_send_sem,
    part_recv_sem,
    right_sems,
    left_sems,
    code_sem,
    square_sems,
    col_sems,
    ready,
):
    me = lax.axis_index("fsdp")
    section = lax.axis_index("section")
    chip = me // CORES
    core = me % CORES
    partner = chip * CORES + (1 - core)
    right = ((chip + 1) % chips) * CORES + core
    left = ((chip + chips - 1) % chips) * CORES + core
    cols = total.shape[-1]
    items = (chips - 1) * slabs

    def own_copy(dest, slab):
        return pltpu.make_async_copy(
            grads.at[dest, core, slab], own.at[dest, slab], own_sem.at[dest * slabs + slab]
        )

    def part_copy(dest, slab):
        return pltpu.make_async_remote_copy(
            src_ref=grads.at[dest, 1 - core, slab],
            dst_ref=part.at[dest, slab],
            send_sem=part_send_sem.at[dest * slabs + slab],
            recv_sem=part_recv_sem.at[dest * slabs + slab],
            device_id={"fsdp": partner},
            device_id_type=pl.DeviceIdType.MESH,
        )

    def hop(wire, tops, sems, slot, target):
        return tuple(
            pltpu.make_async_remote_copy(
                src_ref=ref.at[slot],
                dst_ref=ref.at[slot],
                send_sem=sems.at[2 * kind, slot],
                recv_sem=sems.at[2 * kind + 1, slot],
                device_id={"fsdp": target},
                device_id_type=pl.DeviceIdType.MESH,
            )
            for kind, ref in enumerate((wire, tops))
        )

    def right_slot(dest, slab):
        return (dest - 1) * slabs + slab

    def left_slot(dest, slab):
        return dest * slabs + slab

    def right_hop(slot):
        return hop(right_code, right_top, right_sems, slot, right)

    def left_hop(slot):
        return hop(left_code, left_top, left_sems, slot, left)

    def start(copies):
        for copy in copies:
            copy.start()

    def wait_recv(copies):
        for copy in copies:
            copy.wait_recv()

    def piece_rows(i):
        return pl.ds(pl.multiple_of(i * PIECE, PIECE), PIECE)

    def encode(term, wire, tops, slot):
        def collect(i, high):
            rows = piece_rows(i)
            value = term(rows)
            stage[rows, :] = value
            return jnp.maximum(
                high, jnp.max(jnp.abs(value).reshape(PIECE // 8, 8, cols), axis=0)
            )

        high = lax.fori_loop(0, SLAB // PIECE, collect, jnp.zeros((8, cols), F32))
        top = jnp.maximum(jnp.max(high, axis=0, keepdims=True), TINY)
        tops[slot] = top
        gain = LEVELS * lax.rsqrt(top)

        @pl.loop(0, SLAB // PIECE)
        def _(i):
            rows = piece_rows(i)
            value = stage[rows, :]
            root = value * lax.rsqrt(jnp.maximum(jnp.abs(value), TINY))
            wire[slot, rows, :] = jnp.round(root * gain).astype(jnp.int32).astype(jnp.int16)

    def decoder(wire, tops, slot):
        unit = tops[slot] * (1.0 / (LEVELS * LEVELS))

        def decode(rows):
            code = wire[slot, rows, :].astype(jnp.int32).astype(F32)
            return code * jnp.abs(code) * unit

        return decode

    def add_total(slab, decode):
        @pl.loop(0, SLAB // PIECE)
        def _(i):
            rows = piece_rows(i)
            total[slab, rows, :] += decode(rows)

    def wait_pair(dest, slab):
        own_copy(dest, slab).wait()
        part_copy(dest, slab).wait_recv()

    def pair_sum(dest, slab):
        def term(rows):
            return own[dest, slab, rows, :].astype(F32) + part[dest, slab, rows, :].astype(F32)

        return term

    def joined(decode, pair):
        return lambda rows: decode(rows) + pair(rows)

    def in_order(i):
        step, slab = i // slabs, i % slabs
        return jnp.where(2 * chip < chips, chips - 1 - step, step), slab

    def section_peer(s):
        return {"section": (section + s) % sections}

    def greet(semaphore, device):
        pl.semaphore_signal(
            semaphore, inc=1, device_id=device, device_id_type=pl.DeviceIdType.MESH
        )

    barrier = pltpu.get_barrier_semaphore()
    greet(barrier, {"fsdp": partner})
    for s in range(1, sections):
        greet(barrier, section_peer(s))

    @pl.when(chip > 0)
    def _():
        greet(barrier, {"fsdp": left})

    @pl.when(chip < chips - 1)
    def _():
        greet(barrier, {"fsdp": right})

    @pl.loop(0, chips * slabs)
    def _(i):
        own_copy(*in_order(i)).start()

    ends = (chip == 0).astype(jnp.int32) + (chip == chips - 1).astype(jnp.int32)
    pl.semaphore_wait(barrier, sections + 2 - ends)

    @pl.loop(0, chips * slabs)
    def _(i):
        part_copy(*in_order(i)).start()

    code_copies = (
        pltpu.make_async_copy(first_codes, codes_a, code_sem.at[0]),
        pltpu.make_async_copy(second_codes, codes_b, code_sem.at[1]),
    )
    for copy in code_copies:
        copy.start()

    @pl.when(chip == 0)
    def _():
        @pl.loop(0, items)
        def _(j):
            dest, slab = chips - 1 - j // slabs, j % slabs
            wait_pair(dest, slab)
            slot = right_slot(dest, slab)
            encode(pair_sum(dest, slab), right_code, right_top, slot)
            start(right_hop(slot))

    @pl.when(chip == chips - 1)
    def _():
        @pl.loop(0, items)
        def _(j):
            dest, slab = j // slabs, j % slabs
            wait_pair(dest, slab)
            slot = left_slot(dest, slab)
            encode(pair_sum(dest, slab), left_code, left_top, slot)
            start(left_hop(slot))

    @pl.loop(0, slabs)
    def _(slab):
        wait_pair(chip, slab)
        term = pair_sum(chip, slab)

        @pl.loop(0, SLAB // PIECE)
        def _(i):
            rows = piece_rows(i)
            total[slab, rows, :] = term(rows)

    for copy in code_copies:
        copy.wait()

    @pl.loop(0, slabs)
    def _(slab):
        rows = pl.ds(pl.multiple_of(slab * SLAB, SLAB), SLAB)
        first_row = jnp.broadcast_to(first_rows[:, rows], (LANES, SLAB)).T
        second_row = jnp.broadcast_to(second_rows[:, rows], (LANES, SLAB)).T
        for q in range(cols // LANES):
            span = pl.ds(q * LANES, LANES)
            first_bound = jnp.minimum(first_row, first_cols[:, span])
            second_bound = jnp.minimum(second_row, second_cols[:, span])
            first_old = codes_a[slab, :, span].astype(F32) / 7.0 * first_bound
            second_old = codes_b[slab, :, span].astype(F32) / 15.0 * second_bound
            first[slab, :, span] = beta_first * first_old
            second[slab, :, span] = beta_second * second_old

    right_lag = LAG * chip
    left_lag = LAG * (chips - 1 - chip)

    @pl.loop(0, items + LAG * (chips - 1))
    def _(step):
        @pl.when(step == LAG * chips)
        def _():
            for s in range(1, sections):
                greet(ready, section_peer(s))

        j = step - right_lag
        dest = chips - 1 - j // slabs
        slab = j % slabs

        @pl.when((chip > 0) & (j >= 0) & (dest >= chip))
        def _():
            slot = right_slot(dest, slab)
            wait_recv(right_hop(slot))
            decode = decoder(right_code, right_top, slot)

            @pl.when(dest > chip)
            def _():
                wait_pair(dest, slab)
                encode(joined(decode, pair_sum(dest, slab)), right_code, right_top, slot)
                start(right_hop(slot))

            @pl.when(dest == chip)
            def _():
                add_total(slab, decode)

        i = step - left_lag
        low = i // slabs
        strip = i % slabs

        @pl.when((chip < chips - 1) & (i >= 0) & (low <= chip))
        def _():
            slot = left_slot(low, strip)
            wait_recv(left_hop(slot))
            decode = decoder(left_code, left_top, slot)

            @pl.when(low < chip)
            def _():
                wait_pair(low, strip)
                encode(joined(decode, pair_sum(low, strip)), left_code, left_top, slot)
                start(left_hop(slot))

            @pl.when(low == chip)
            def _():
                add_total(strip, decode)

    pieces = SLAB // PIECE

    def fold(value):
        return value.reshape(PIECE // 8, 8, cols)

    def add_squares(i, acc):
        g = total[i // pieces, piece_rows(i % pieces), :]
        return acc + jnp.sum(fold(g * g), axis=0)

    squares = lax.fori_loop(
        0, slabs * pieces, add_squares, jnp.zeros((8, cols), F32), unroll=UNROLL
    )
    folded = squares[:, :LANES]
    for q in range(1, cols // LANES):
        folded = folded + squares[:, q * LANES : (q + 1) * LANES]
    folded = jnp.sum(folded, axis=0, keepdims=True)

    def to_all(axis, size, position, source, slots, sems):
        copies = [
            pltpu.make_async_remote_copy(
                src_ref=source,
                dst_ref=slots.at[s - 1],
                send_sem=sems.at[0, s - 1],
                recv_sem=sems.at[1, s - 1],
                device_id={axis: (position + s) % size},
                device_id_type=pl.DeviceIdType.MESH,
            )
            for s in range(1, size)
        ]
        for copy in copies:
            copy.start()
        return copies

    def square_copy(k):
        return pltpu.make_async_remote_copy(
            src_ref=square_send,
            dst_ref=square_recv.at[k - 1],
            send_sem=square_sems.at[0, k - 1],
            recv_sem=square_sems.at[1, k - 1],
            device_id={
                "section": (section + k // fsdp) % sections,
                "fsdp": (me + k % fsdp) % fsdp,
            },
            device_id_type=pl.DeviceIdType.MESH,
        )

    def add_square(k, acc):
        square_copy(k).wait_recv()
        return acc + square_recv[k - 1]

    square_send[...] = folded
    pl.semaphore_wait(ready, sections - 1)
    devices = sections * fsdp

    @pl.loop(1, devices)
    def _(k):
        square_copy(k).start()

    folded = lax.fori_loop(1, devices, add_square, folded)
    square_sum = jnp.sum(folded, axis=1, keepdims=True)
    norm = jnp.sqrt(jnp.broadcast_to(square_sum, (1, cols)))
    scale = clip_limit / jnp.maximum(norm, clip_limit)
    first_gain = (1.0 - beta_first) * scale
    second_gain = (1.0 - beta_second) * scale * scale

    def moments(slab, rows):
        g = total[slab, rows, :]
        first_new = first[slab, rows, :] + first_gain * g
        second_new = second[slab, rows, :] + second_gain * g * g
        return first_new, second_new

    def raise_tops(i, carry):
        first_top, second_top = carry
        first_new, second_new = moments(i // pieces, piece_rows(i % pieces))
        first_top = jnp.maximum(first_top, jnp.max(fold(jnp.abs(first_new)), axis=0))
        second_top = jnp.maximum(second_top, jnp.max(fold(second_new), axis=0))
        return first_top, second_top

    nothing = jnp.zeros((8, cols), F32)
    first_top, second_top = lax.fori_loop(
        0, slabs * pieces, raise_tops, (nothing, nothing), unroll=UNROLL
    )
    first_top = jnp.max(first_top, axis=0, keepdims=True)
    second_top = jnp.max(second_top, axis=0, keepdims=True)
    col_send[0:1, :] = first_top
    col_send[1:2, :] = second_top
    col_copies = to_all("fsdp", fsdp, me, col_send, col_recv, col_sems)

    def lane_peak(block):
        peak = block[:, :LANES]
        for q in range(1, cols // LANES):
            peak = jnp.maximum(peak, block[:, q * LANES : (q + 1) * LANES])
        return peak

    @pl.loop(0, slabs)
    def _(slab):
        @pl.loop(0, pieces, unroll=UNROLL)
        def _(i):
            rows = piece_rows(i)
            first_new, second_new = moments(slab, rows)
            first[slab, rows, :] = first_new
            second[slab, rows, :] = second_new
            direction[slab, rows, :] = first_new / (jnp.sqrt(second_new) + epsilon)
            first_peak[rows, :] = lane_peak(jnp.abs(first_new))
            second_peak[rows, :] = lane_peak(second_new)

        span = pl.ds(pl.multiple_of(slab * SLAB, SLAB), SLAB)
        first_row = jnp.max(first_peak[...], axis=1, keepdims=True)
        first_row = jnp.broadcast_to(jnp.maximum(first_row, scale_floor), (SLAB, LANES))
        second_row = jnp.max(second_peak[...], axis=1, keepdims=True)
        second_row = jnp.broadcast_to(second_row, (SLAB, LANES))
        first_inverse[slab] = 1.0 / first_row
        second_inverse[slab] = 1.0 / second_row
        first_rowmax[:, span] = first_row.T[0:1, :]
        second_rowmax[:, span] = second_row.T[0:1, :]

    @pl.loop(0, chips * slabs)
    def _(i):
        part_copy(i // slabs, i % slabs).wait_send()

    @pl.loop(0, items)
    def _(j):
        slab = j % slabs

        @pl.when(j // slabs + 1 > chip)
        def _():
            for copy in right_hop(right_slot(j // slabs + 1, slab)):
                copy.wait_send()

        @pl.when(j // slabs < chip)
        def _():
            for copy in left_hop(left_slot(j // slabs, slab)):
                copy.wait_send()

    @pl.loop(1, devices)
    def _(k):
        square_copy(k).wait_send()

    for s, copy in enumerate(col_copies):
        copy.wait_recv()
        first_top = jnp.maximum(first_top, col_recv[s, 0:1, :])
        second_top = jnp.maximum(second_top, col_recv[s, 1:2, :])
    first_colmax[...] = jnp.maximum(first_top, scale_floor)
    second_colmax[...] = second_top
    for copy in col_copies:
        copy.wait_send()


def finish_kernel(
    direction,
    first,
    second,
    first_inverse,
    second_inverse,
    first_rowmax,
    second_rowmax,
    first_colmax,
    second_colmax,
    direction_out,
    first_out,
    second_out,
    first_row_out,
    first_col_out,
    second_row_out,
    second_col_out,
    first_scaled,
    second_scaled,
    direction_sem,
    out_sem,
    small_sem,
):
    slabs, _, cols = first.shape
    small = (
        (first_rowmax, first_row_out),
        (first_colmax, first_col_out),
        (second_rowmax, second_row_out),
        (second_colmax, second_col_out),
    )
    copies = [
        pltpu.make_async_copy(direction.at[slab], direction_out.at[slab], direction_sem.at[slab])
        for slab in range(slabs)
    ]
    copies += [
        pltpu.make_async_copy(source, target, small_sem.at[i])
        for i, (source, target) in enumerate(small)
    ]
    for copy in copies:
        copy.start()
    first_col = 1.0 / first_colmax[...]
    second_col = 1.0 / second_colmax[...]

    def out_copies(slab):
        return (
            pltpu.make_async_copy(first_scaled.at[slab], first_out.at[slab], out_sem.at[0, slab]),
            pltpu.make_async_copy(
                second_scaled.at[slab], second_out.at[slab], out_sem.at[1, slab]
            ),
        )

    @pl.loop(0, slabs)
    def _(slab):
        @pl.loop(0, SLAB // PIECE, unroll=UNROLL)
        def _(i):
            rows = pl.ds(pl.multiple_of(i * PIECE, PIECE), PIECE)
            first_row = first_inverse[slab, rows, :]
            second_row = second_inverse[slab, rows, :]
            for q in range(cols // LANES):
                span = slice(q * LANES, (q + 1) * LANES)
                first_scaled[slab, rows, span] = first[slab, rows, span] * jnp.maximum(
                    first_row, first_col[:, span]
                )
                second_scaled[slab, rows, span] = second[slab, rows, span] * jnp.maximum(
                    second_row, second_col[:, span]
                )

        for copy in out_copies(slab):
            copy.start()

    for copy in copies:
        copy.wait()

    @pl.loop(0, slabs)
    def _(slab):
        for copy in out_copies(slab):
            copy.wait()


def local(
    grad_parts, first_codes, first_rows, first_columns, second_codes, second_rows, second_columns
):
    fsdp = lax.axis_size("fsdp")
    sections = lax.axis_size("section")
    layers, _, row_count, cols = grad_parts.shape
    chips = fsdp // CORES
    rows = row_count // fsdp
    slabs = rows // SLAB
    clip_limit = clip_rms * math.sqrt(layers * sections * row_count * cols)
    grads = grad_parts.reshape(chips, CORES, slabs, SLAB, cols)
    tiled = (slabs, SLAB, cols)
    items = (chips - 1) * slabs
    hbm = pl.BlockSpec(memory_space=pl.ANY)
    vmem = pl.BlockSpec(memory_space=pltpu.VMEM)
    dma = pltpu.SemaphoreType.DMA
    inverse = (slabs, SLAB, LANES)
    kept = (tiled, tiled, tiled, inverse, inverse, (1, rows), (1, rows), (1, cols), (1, cols))
    held = pl.pallas_call(
        functools.partial(exchange_kernel, chips, fsdp, sections, slabs, clip_limit),
        out_shape=tuple(pltpu.VMEM(shape, F32) for shape in kept),
        in_specs=[hbm, hbm, vmem, vmem, hbm, vmem, vmem],
        out_specs=(vmem,) * len(kept),
        scratch_shapes=[
            pltpu.VMEM((chips, *tiled), jnp.bfloat16),
            pltpu.VMEM((chips, *tiled), jnp.bfloat16),
            pltpu.VMEM((items, SLAB, cols), jnp.int16),
            pltpu.VMEM((items, SLAB, cols), jnp.int16),
            pltpu.VMEM((items, 1, cols), F32),
            pltpu.VMEM((items, 1, cols), F32),
            pltpu.VMEM((SLAB, cols), F32),
            pltpu.VMEM(tiled, F32),
            pltpu.VMEM(tiled, jnp.int32),
            pltpu.VMEM(tiled, jnp.int32),
            pltpu.VMEM((SLAB, LANES), F32),
            pltpu.VMEM((SLAB, LANES), F32),
            pltpu.VMEM((1, LANES), F32),
            pltpu.VMEM((sections * fsdp - 1, 1, LANES), F32),
            pltpu.VMEM((2, cols), F32),
            pltpu.VMEM((fsdp - 1, 2, cols), F32),
            dma((chips * slabs,)),
            dma((chips * slabs,)),
            dma((chips * slabs,)),
            dma((4, items)),
            dma((4, items)),
            dma((2,)),
            dma((2, sections * fsdp - 1)),
            dma((2, fsdp - 1)),
            pltpu.SemaphoreType.REGULAR,
        ],
        compiler_params=pltpu.CompilerParams(
            has_side_effects=True, collective_id=0, vmem_limit_bytes=EXCHANGE_VMEM
        ),
    )(
        grads,
        first_codes.reshape(tiled),
        first_rows,
        first_columns,
        second_codes.reshape(tiled),
        second_rows,
        second_columns,
    )
    finished = pl.pallas_call(
        finish_kernel,
        out_shape=(
            jax.ShapeDtypeStruct(tiled, F32),
            jax.ShapeDtypeStruct(tiled, F32),
            jax.ShapeDtypeStruct(tiled, F32),
            jax.ShapeDtypeStruct((1, rows), F32),
            jax.ShapeDtypeStruct((1, cols), F32),
            jax.ShapeDtypeStruct((1, rows), F32),
            jax.ShapeDtypeStruct((1, cols), F32),
        ),
        in_specs=[vmem] * len(kept),
        out_specs=(hbm,) * 7,
        scratch_shapes=[
            pltpu.VMEM(tiled, F32),
            pltpu.VMEM(tiled, F32),
            dma((slabs,)),
            dma((2, slabs)),
            dma((4,)),
        ],
        compiler_params=pltpu.CompilerParams(vmem_limit_bytes=FINISH_VMEM),
    )(*(pltpu.with_memory_space_constraint(x, pltpu.VMEM) for x in held))
    direction, first_scaled, second_scaled = finished[:3]
    first_rowmax, first_colmax, second_rowmax, second_colmax = finished[3:]
    shape = (layers, rows, cols)
    return (
        direction.reshape(shape),
        first_scaled.reshape(shape),
        second_scaled.reshape(shape),
        first_rowmax,
        first_colmax,
        second_rowmax,
        second_colmax,
    )


def solution(mesh):
    placed = (
        P("section", "fsdp", None, None),
        P("section", "fsdp", None),
        P("section", "fsdp"),
        P("section", None),
        P("section", "fsdp", None),
        P("section", "fsdp"),
        P("section", None),
    )
    return jax.shard_map(
        local,
        mesh=mesh,
        in_specs=placed,
        out_specs=(
            P("section", "fsdp", None),
            P("section", "fsdp", None),
            P("section", "fsdp", None),
            P("section", "fsdp"),
            P("section", None),
            P("section", "fsdp"),
            P("section", None),
        ),
        check_vma=False,
    )
```
